256 devices in a mesh: wide: 32 (over x, y, core), narrow: 8 (over z).
Axes of the slice: x: 4, y: 4, z: 8, core: 2. Of those that a mesh axis runs over, the one named last changes fastest.
Arguments:
- row_vectors: bfloat16 [32768, 2048], P('wide'), may hold values from -0.59765625 to 1.3984375
- col_vectors: bfloat16 [4096, 2048], P('narrow', 'wide'), may hold values from -0.59765625 to 1.3984375
- primal_matrix: bfloat16 [2048, 2048], P('wide'), may hold values from -1 to 3, as said below
- dual_inverse: bfloat16 [2048, 2048], P('wide'), may hold values from -1 to 3, as said below
Outputs:
- factored: float32 [32768, 4096], P('wide', 'narrow')
The draws below stay inside these ranges and needn't reach their ends.
Inputs may be any that keep to these rules, and one draw needn't show every extreme that they name: `primal_matrix`: symmetric positive definite. `dual_inverse`: symmetric positive definite.
All inputs are finite; a program needn't handle non-finite values.
Results may differ from the reference program's by a relative error of at most 0.0027.
Values may be sent and summed in bfloat16 or wider, within the bound.
A program may use at most 64 MiB of HBM per device.

```python
import math
import jax
import jax.numpy as jnp
from jax import lax

N = 2048
PANEL = 512
ROWS = 32768
COLS = 4096


def draw_definite(key, salt_value):
    base_key = jax.random.fold_in(key, salt_value)
    key_diag, key_off = jax.random.split(base_key)
    diag_values = jnp.exp(jax.random.uniform(key_diag, (N,), jnp.float32, math.log(0.6), math.log(2.4)))
    off_part = jax.random.normal(key_off, (N, N), jnp.float32) * (0.25 / math.sqrt(N))
    sym_part = (off_part + off_part.T) * 0.5
    return (jnp.diag(diag_values) + sym_part).astype(jnp.bfloat16)


def draw_primal_matrix(key, part):
    return draw_definite(key, 11)


def draw_dual_inverse(key, part):
    return draw_definite(key, 23)


def level_of(stream_key, dims, cuts, least, largest):
    def one(position, blocks):
        steps = jax.random.uniform(jax.random.fold_in(jax.random.fold_in(stream_key, 6), position), (blocks,), jnp.float32, least / len(cuts), largest / len(cuts))
        return jnp.repeat(jnp.exp(steps), dims[position] // blocks).reshape((-1,) + (1,) * (len(dims) - position - 1))

    factor_of = one(*cuts[0])
    for cut in cuts[1:]:
        factor_of = factor_of * one(*cut)
    return factor_of


def setup_inputs(seed: int = 0) -> dict:
    seeds = jax.random.split(jax.random.key(seed), 5)
    row_vectors = jnp.clip(-0.59765625 + 1.9960938 * jax.random.uniform(seeds[0], (ROWS, N), jnp.float32) ** level_of(seeds[0], (ROWS, N), ((0, 32),), -0.2, 0.2), -0.59765625, 1.3984375).astype(jnp.bfloat16)
    col_vectors = jnp.clip(-0.59765625 + 1.9960938 * jax.random.uniform(seeds[1], (COLS, N), jnp.float32) ** level_of(seeds[1], (COLS, N), ((0, 8), (1, 32)), -0.2, 0.2), -0.59765625, 1.3984375).astype(jnp.bfloat16)
    primal_matrix = draw_primal_matrix(jax.random.fold_in(seeds[4], 71), 0)
    dual_inverse = draw_dual_inverse(jax.random.fold_in(seeds[4], 71), 0)
    return {"row_vectors": row_vectors, "col_vectors": col_vectors, "primal_matrix": primal_matrix, "dual_inverse": dual_inverse}


def reference(row_vectors, col_vectors, primal_matrix, dual_inverse):
    cone_order = primal_matrix.shape[0]
    gram_scale = 16.0 / (cone_order * cone_order)
    prod_primal = jnp.dot(primal_matrix.astype(jnp.float32), col_vectors.T.astype(jnp.float32), preferred_element_type=jnp.float32).astype(jnp.bfloat16)
    prod_dual = jnp.dot(dual_inverse.astype(jnp.float32), col_vectors.T.astype(jnp.float32), preferred_element_type=jnp.float32).astype(jnp.bfloat16)
    gram_primal = jnp.dot(row_vectors.astype(jnp.float32), prod_primal.astype(jnp.float32), preferred_element_type=jnp.float32)
    gram_dual = jnp.dot(row_vectors.astype(jnp.float32), prod_dual.astype(jnp.float32), preferred_element_type=jnp.float32)
    slab = gram_primal * gram_dual * gram_scale
    panel_set = col_vectors[:PANEL]
    gram = jnp.dot(panel_set.astype(jnp.float32), prod_primal.astype(jnp.float32), preferred_element_type=jnp.float32) * jnp.dot(panel_set.astype(jnp.float32), prod_dual.astype(jnp.float32), preferred_element_type=jnp.float32) * gram_scale
    factor = jnp.linalg.cholesky(gram[:, :PANEL])
    solved = jax.scipy.linalg.solve_triangular(factor, gram, lower=True)
    panel_cols = jax.scipy.linalg.solve_triangular(factor, slab[:, :PANEL].T, lower=True).T
    trailing = slab[:, PANEL:] - jnp.dot(panel_cols, solved[:, PANEL:], precision=lax.Precision.HIGHEST)
    return jnp.concatenate([panel_cols, trailing], axis=1)
```

```python
import jax
import jax.numpy as jnp
from jax import lax
from jax.experimental import pallas as pl
from jax.experimental.pallas import tpu as pltpu
from jax.sharding import PartitionSpec as P

F32 = jnp.float32
BF16 = jnp.bfloat16
HIGHEST = lax.Precision.HIGHEST
MESH = pl.DeviceIdType.MESH
SIDE = 4
TILE = 128


def lane_copy(x, k):
    return jnp.take_along_axis(x, jnp.full(x.shape, k, jnp.int32), axis=1)


def row_copy(x, r):
    return jnp.broadcast_to(x[r : r + 1, :], x.shape)


def split(x):
    hi = x.astype(BF16)
    return hi, (x - hi.astype(F32)).astype(BF16)


def dot(a, b):
    return jnp.dot(a, b, preferred_element_type=F32)


def dot_first(a, b):
    return lax.dot_general(a, b, (((0,), (0,)), ((), ())), preferred_element_type=F32)


def factor_tile(tile):
    groups = TILE // 8
    lanes = lax.broadcasted_iota(jnp.int32, (8, TILE), 1)
    rows = lax.broadcasted_iota(jnp.int32, (8, TILE), 0)
    left = [tile[8 * g : 8 * g + 8, :] for g in range(groups)]
    right = [(lanes == rows + 8 * g).astype(F32) for g in range(groups)]
    for s in range(groups):
        cols = {g: [lane_copy(left[g], 8 * s + j) for j in range(8)] for g in range(s, groups)}
        scale = jnp.zeros((8, TILE), F32)
        for j in range(8):
            pivot = row_copy(cols[s][j], j)
            inv = 1.0 / pivot
            lead_left, lead_right = row_copy(left[s], j), row_copy(right[s], j)
            lead_cols = [row_copy(cols[s][k], j) for k in range(j + 1, 8)]
            scale = jnp.where(rows == j, pivot, scale)
            for g in range(s, groups):
                mult = cols[g][j] * inv
                if g == s:
                    mult = jnp.where(rows > j, mult, 0.0)
                left[g] = left[g] - mult * lead_left
                right[g] = right[g] - mult * lead_right
                for k in range(j + 1, 8):
                    cols[g][k] = cols[g][k] - mult * lead_cols[k - j - 1]
        tile[8 * s : 8 * s + 8, :] = right[s] * lax.rsqrt(scale)


def factor_block(aug, tile, b):
    size = aug.shape[0]
    at = pl.ds(pl.multiple_of(b * TILE, TILE), TILE)
    tile[...] = aug[at, at]
    factor_tile(tile)
    rows = lax.broadcasted_iota(jnp.int32, (TILE, TILE), 0)
    lanes = lax.broadcasted_iota(jnp.int32, (TILE, TILE), 1)
    aug[at, at] = (rows == lanes).astype(F32)
    aug[at, :] = jnp.dot(tile[...], aug[at, :], precision=HIGHEST, preferred_element_type=F32)

    def below(i, _):
        to = pl.ds(pl.multiple_of(i * TILE, TILE), TILE)
        coef = aug[at, to]
        aug[to, at] = jnp.zeros((TILE, TILE), F32)
        aug[to, :] = aug[to, :] - lax.dot_general(
            coef, aug[at, :], (((0,), (0,)), ((), ())), precision=HIGHEST, preferred_element_type=F32
        )
        return 0

    lax.fori_loop(b + 1, size // TILE, below, 0)


class Gather:
    def __init__(self, view, share, sems):
        self.view, self.share, self.sems = view, share, sems
        wide, self.narrow = lax.axis_index("wide"), lax.axis_index("narrow")
        self.core = lax.rem(wide, 2)
        x, y = wide // 8, lax.rem(wide // 2, SIDE)
        self.step_p, self.step_q = 2 + 6 * self.core, 8 - 6 * self.core
        self.p = y + self.core * (x - y)
        self.q = x + self.core * (y - x)
        self.partner = wide + 1 - 2 * self.core

    def around(self, value, by):
        return lax.rem(value + by, SIDE)

    def wide(self, dp, dq):
        p, q = self.around(self.p, dp), self.around(self.q, dq)
        return p * self.step_p + q * self.step_q + self.core

    def rows(self, dp, dq, half=None):
        start, count = self.wide(dp, dq) * self.share, self.share
        if half is not None:
            count = self.share // 2
            start = start + half * count
        return self.view(pl.ds(pl.multiple_of(start, count), count))

    def send(self, ref, to, sem):
        pltpu.make_async_remote_copy(
            src_ref=ref, dst_ref=ref, send_sem=self.sems.at[16], recv_sem=self.sems.at[sem],
            device_id=(to, self.narrow), device_id_type=MESH,
        ).start()

    def got(self, ref, sem):
        pltpu.make_async_remote_copy(
            src_ref=ref, dst_ref=ref, send_sem=self.sems.at[16], recv_sem=self.sems.at[sem],
            device_id=(self.partner, self.narrow), device_id_type=MESH,
        ).wait_recv()

    def second(self, dp, k):
        ref = self.rows(dp, 0)
        self.send(ref, self.wide(0, 1), 3 + k)
        self.send(ref, self.wide(0, 3), 7 + k)
        self.send(ref, self.partner, 15)

    def own(self):
        ref = self.rows(0, 0)
        self.send(ref, self.wide(1, 0), 0)
        self.send(ref, self.wide(3, 0), 1)
        self.second(0, 0)

    def first_near(self):
        for side, (dp, to) in enumerate(((3, 1), (1, 3))):
            self.got(self.rows(dp, 0), side)
            self.send(self.rows(dp, 0, side), self.wide(to, 0), 2)
            self.second(dp, 1 + side)

    def first_far(self):
        self.got(self.rows(2, 0), 2)
        self.second(2, 3)

    def second_near(self, ks=(0, 1, 2, 3)):
        for k in ks:
            dp = (0, 3, 1, 2)[k]
            for side, (dq, to) in enumerate(((3, 1), (1, 3))):
                self.got(self.rows(dp, dq), 3 + 4 * side + k)
                self.send(self.rows(dp, dq, side), self.wide(0, to), 11 + k)
                self.send(self.rows(dp, dq), self.partner, 15)

    def second_far(self):
        for k, dp in enumerate((0, 3, 1, 2)):
            self.got(self.rows(dp, 2), 11 + k)
            self.send(self.rows(dp, 2), self.partner, 15)

    def last(self):
        self.got(self.view(pl.ds(0, 16 * self.share)), 15)

    def sent(self):
        ref = self.view(pl.ds(0, 31 * self.share))
        pltpu.make_async_remote_copy(
            src_ref=ref, dst_ref=ref, send_sem=self.sems.at[16], recv_sem=self.sems.at[15],
            device_id=(self.partner, self.narrow), device_id_type=MESH,
        ).wait_send()


def kernel(
    row_ref, col_ref, primal_ref, dual_ref, out_ref,
    rows_v, both_v, cols_v, prods_v, panel_v, aug, tile, gram_v,
    first_hi, first_lo, slab_v, inv_hi, inv_lo, mid_hi, mid_lo, mix_hi, mix_lo,
    sems, z_sems, in_sems, out_sems,
):
    wide, narrow = lax.axis_index("wide"), lax.axis_index("narrow")
    planes = lax.axis_size("narrow")
    order = rows_v.shape[1]
    panel = gram_v.shape[0]
    share = both_v.shape[0] // 2
    scale = 16.0 / (order * order)

    load_rows = pltpu.make_async_copy(row_ref, rows_v, in_sems.at[0])
    load_primal = pltpu.make_async_copy(primal_ref, both_v.at[pl.ds(0, share)], in_sems.at[1])
    load_dual = pltpu.make_async_copy(dual_ref, both_v.at[pl.ds(share, share)], in_sems.at[2])
    load_primal.start()
    load_dual.start()
    load_rows.start()

    mine = pl.ds(pl.multiple_of(wide * share, share), share)
    shard = col_ref[...].T
    cols_v[1, mine, :] = shard

    @pl.when(narrow == 0)
    def _():
        cols_v[0, mine, :] = shard

    panel_cols = Gather(lambda r: cols_v.at[0, r], share, sems.at[0])
    block_cols = Gather(lambda r: cols_v.at[1, r], share, sems.at[1])
    panel_prods = Gather(lambda r: prods_v.at[0, :, r], share, sems.at[2])
    block_prods = Gather(lambda r: prods_v.at[1, :, r], share, sems.at[3])

    barrier = pltpu.get_barrier_semaphore()
    g = panel_cols
    for to in (g.wide(1, 0), g.wide(3, 0), g.wide(0, 1), g.wide(0, 3), g.partner):
        pl.semaphore_signal(barrier, inc=1, device_id=(to, narrow), device_id_type=MESH)

    @pl.when(narrow == 0)
    def _():
        for z in range(1, planes):
            pl.semaphore_signal(barrier, inc=1, device_id=(wide, z), device_id_type=MESH)
        pl.semaphore_wait(barrier, 5 + planes - 1)

    @pl.when(narrow != 0)
    def _():
        pl.semaphore_signal(barrier, inc=1, device_id=(wide, 0), device_id_type=MESH)
        pl.semaphore_wait(barrier, 6)

    def z_copy(z):
        ref = cols_v.at[0, mine]
        return pltpu.make_async_remote_copy(
            src_ref=ref, dst_ref=ref, send_sem=z_sems.at[0], recv_sem=z_sems.at[1],
            device_id=(wide, z), device_id_type=MESH,
        )

    @pl.when(narrow == 0)
    def _():
        for z in (4, 3, 5, 2, 6, 1, 7):
            z_copy(z).start()

    block_cols.own()
    block_cols.first_near()

    @pl.when(narrow != 0)
    def _():
        z_copy(0).wait_recv()

    panel_cols.own()
    block_cols.first_far()
    panel_cols.first_near()
    block_cols.second_near()
    panel_cols.first_far()
    block_cols.second_far()
    panel_cols.second_near()
    panel_cols.second_far()

    def products(which):
        done = dot(both_v[...], cols_v[which]).astype(BF16)
        prods_v[which, 0, mine, :] = done[:share]
        prods_v[which, 1, mine, :] = done[share:]

    load_primal.wait()
    load_dual.wait()
    panel_cols.last()
    products(0)
    panel_prods.own()
    block_cols.last()
    products(1)
    panel_prods.first_near()
    block_prods.own()

    def turn(t, _):
        at = pl.ds(pl.multiple_of(t * TILE, TILE), TILE)
        panel_v[:, at] = cols_v[0, at, :].T
        return 0

    lax.fori_loop(0, order // TILE, turn, 0)

    panel_prods.first_far()
    block_prods.first_near()
    panel_prods.second_near()
    block_prods.first_far()
    panel_prods.second_far()
    panel_prods.last()

    def hadamard(lhs, which):
        return dot(lhs, prods_v[which, 0]) * dot(lhs, prods_v[which, 1]) * scale

    step = 256

    def each(count, body):
        def one(t, _):
            body(pl.ds(pl.multiple_of(t * step, step), step))
            return 0

        lax.fori_loop(0, count // step, one, 0)

    @lambda body: each(panel, body)
    def _(at):
        aug[at, :] = hadamard(panel_v[at, :], 0)

    def chol(b, _):
        factor_block(aug, tile, b)

        @pl.when(b == 0)
        def _():
            block_prods.second_near()

        @pl.when(b == 1)
        def _():
            block_prods.second_far()

        return 0

    lax.fori_loop(0, panel // TILE, chol, 0)

    load_rows.wait()

    @lambda body: each(rows_v.shape[0], body)
    def _(at):
        first_hi[at, :], first_lo[at, :] = split(hadamard(rows_v[at, :], 0))

    block_prods.last()

    @lambda body: each(panel, body)
    def _(at):
        gram_v[at, :] = hadamard(panel_v[at, :], 1)

    @lambda body: each(rows_v.shape[0], body)
    def _(at):
        slab_v[at, :] = hadamard(rows_v[at, :], 1)

    for b in range(panel // TILE):
        at = pl.ds(b * TILE, TILE)
        lanes = lax.broadcasted_iota(jnp.int32, (TILE, panel), 1)
        kept = jnp.where(lanes < (b + 1) * TILE, aug[at, :], 0.0)
        inv_hi[at, :], inv_lo[at, :] = split(kept)
        gram_hi, gram_lo = split(gram_v[at, :])
        mix_hi[at, :], mix_lo[at, :] = gram_hi, gram_lo

    @lambda body: each(panel, body)
    def _(at):
        solved = dot(inv_hi[at, :], mix_hi[...]) + (
            dot(inv_hi[at, :], mix_lo[...]) + dot(inv_lo[at, :], mix_hi[...])
        )
        rows = lax.broadcasted_iota(jnp.int32, (step, panel), 0) + at.start
        lanes = lax.broadcasted_iota(jnp.int32, (step, panel), 1)
        solved = jnp.where(narrow == 0, jnp.where(rows == lanes, -1.0, 0.0), solved)
        mid_hi[at, :], mid_lo[at, :] = split(solved)

    @lambda body: each(panel, body)
    def _(at):
        mixed = dot_first(inv_hi[:, at], mid_hi[...]) + (
            dot_first(inv_hi[:, at], mid_lo[...]) + dot_first(inv_lo[:, at], mid_hi[...])
        )
        mix_hi[at, :], mix_lo[at, :] = split(mixed)

    @lambda body: each(rows_v.shape[0], body)
    def _(at):
        taken = dot(first_hi[at, :], mix_hi[...]) + (
            dot(first_hi[at, :], mix_lo[...]) + dot(first_lo[at, :], mix_hi[...])
        )
        slab_v[at, :] = jnp.where(narrow == 0, 0.0, slab_v[at, :]) - taken

    store = pltpu.make_async_copy(slab_v, out_ref, out_sems.at[0])
    store.start()
    store.wait()

    for g in (block_cols, panel_cols, panel_prods, block_prods):
        g.sent()

    @pl.when(narrow == 0)
    def _():
        ref = cols_v.at[0, pl.ds(0, (planes - 1) * share)]
        pltpu.make_async_remote_copy(
            src_ref=ref, dst_ref=ref, send_sem=z_sems.at[0], recv_sem=z_sems.at[1],
            device_id=(wide, 1), device_id_type=MESH,
        ).wait_send()


def per_device(row_vectors, col_vectors, primal_matrix, dual_inverse):
    rows, order = row_vectors.shape
    panel = col_vectors.shape[0]
    share = primal_matrix.shape[0]
    whole = pl.BlockSpec(memory_space=pl.ANY)
    small, square = (panel, order), (panel, panel)
    return pl.pallas_call(
        kernel,
        out_shape=jax.ShapeDtypeStruct((rows, panel), F32),
        in_specs=[whole, pl.BlockSpec(memory_space=pltpu.VMEM), whole, whole],
        out_specs=whole,
        scratch_shapes=[
            pltpu.VMEM((rows, order), BF16),
            pltpu.VMEM((2 * share, order), BF16),
            pltpu.VMEM((2, order, panel), BF16),
            pltpu.VMEM((2, 2, order, panel), BF16),
            pltpu.VMEM(small, BF16),
            pltpu.VMEM(square, F32),
            pltpu.VMEM((TILE, TILE), F32),
            pltpu.VMEM(square, F32),
            pltpu.VMEM((rows, panel), BF16),
            pltpu.VMEM((rows, panel), BF16),
            pltpu.VMEM((rows, panel), F32),
            *[pltpu.VMEM(square, BF16)] * 6,
            pltpu.SemaphoreType.DMA((4, 17)),
            pltpu.SemaphoreType.DMA((2,)),
            pltpu.SemaphoreType.DMA((3,)),
            pltpu.SemaphoreType.DMA((1,)),
        ],
        compiler_params=pltpu.CompilerParams(
            collective_id=0, has_side_effects=True, vmem_limit_bytes=58 << 20
        ),
    )(row_vectors, col_vectors, primal_matrix, dual_inverse)


def solution(mesh):
    placed = (P("wide", None), P("narrow", "wide"), P("wide", None), P("wide", None))
    return jax.shard_map(
        per_device, mesh=mesh, in_specs=placed, out_specs=P("wide", "narrow"), check_vma=False
    )
```

```python
import jax
import jax.numpy as jnp
from jax import lax
from jax.experimental import pallas as pl
from jax.experimental.pallas import tpu as pltpu
from jax.sharding import PartitionSpec as P

F32 = jnp.float32
BF16 = jnp.bfloat16
HIGHEST = lax.Precision.HIGHEST
MESH = pl.DeviceIdType.MESH
SIDE = 4
TILE = 128


def lane_copy(x, k):
    return jnp.take_along_axis(x, jnp.full(x.shape, k, jnp.int32), axis=1)


def row_copy(x, r):
    return jnp.broadcast_to(x[r : r + 1, :], x.shape)


def split(x):
    hi = x.astype(BF16)
    return hi, (x - hi.astype(F32)).astype(BF16)


def dot(a, b):
    return jnp.dot(a, b, preferred_element_type=F32)


def dot_first(a, b):
    return lax.dot_general(a, b, (((0,), (0,)), ((), ())), preferred_element_type=F32)


def factor_tile(tile):
    groups = TILE // 8
    lanes = lax.broadcasted_iota(jnp.int32, (8, TILE), 1)
    rows = lax.broadcasted_iota(jnp.int32, (8, TILE), 0)
    left = [tile[8 * g : 8 * g + 8, :] for g in range(groups)]
    right = [(lanes == rows + 8 * g).astype(F32) for g in range(groups)]
    for s in range(groups):
        cols = {g: [lane_copy(left[g], 8 * s + j) for j in range(8)] for g in range(s, groups)}
        scale = jnp.zeros((8, TILE), F32)
        for j in range(8):
            pivot = row_copy(cols[s][j], j)
            inv = 1.0 / pivot
            lead_left, lead_right = row_copy(left[s], j), row_copy(right[s], j)
            lead_cols = [row_copy(cols[s][k], j) for k in range(j + 1, 8)]
            scale = jnp.where(rows == j, pivot, scale)
            for g in range(s, groups):
                mult = cols[g][j] * inv
                if g == s:
                    mult = jnp.where(rows > j, mult, 0.0)
                left[g] = left[g] - mult * lead_left
                right[g] = right[g] - mult * lead_right
                for k in range(j + 1, 8):
                    cols[g][k] = cols[g][k] - mult * lead_cols[k - j - 1]
        tile[8 * s : 8 * s + 8, :] = right[s] * lax.rsqrt(scale)


def factor_block(aug, tile, b, beside):
    size = aug.shape[0]
    at = pl.ds(pl.multiple_of(b * TILE, TILE), TILE)
    tile[...] = aug[at, at]
    beside()
    factor_tile(tile)
    rows = lax.broadcasted_iota(jnp.int32, (TILE, TILE), 0)
    lanes = lax.broadcasted_iota(jnp.int32, (TILE, TILE), 1)
    aug[at, at] = (rows == lanes).astype(F32)
    aug[at, :] = jnp.dot(tile[...], aug[at, :], precision=HIGHEST, preferred_element_type=F32)

    def below(i, _):
        to = pl.ds(pl.multiple_of(i * TILE, TILE), TILE)
        coef = aug[at, to]
        aug[to, at] = jnp.zeros((TILE, TILE), F32)
        aug[to, :] = aug[to, :] - lax.dot_general(
            coef, aug[at, :], (((0,), (0,)), ((), ())), precision=HIGHEST, preferred_element_type=F32
        )
        return 0

    lax.fori_loop(b + 1, size // TILE, below, 0)


class Gather:
    def __init__(self, view, share, sems):
        self.view, self.share, self.sems = view, share, sems
        wide, self.narrow = lax.axis_index("wide"), lax.axis_index("narrow")
        self.core = lax.rem(wide, 2)
        x, y = wide // 8, lax.rem(wide // 2, SIDE)
        self.step_p, self.step_q = 2 + 6 * self.core, 8 - 6 * self.core
        self.p = y + self.core * (x - y)
        self.q = x + self.core * (y - x)
        self.partner = wide + 1 - 2 * self.core

    def around(self, value, by):
        return lax.rem(value + by, SIDE)

    def wide(self, dp, dq):
        p, q = self.around(self.p, dp), self.around(self.q, dq)
        return p * self.step_p + q * self.step_q + self.core

    def rows(self, dp, dq, half=None):
        start, count = self.wide(dp, dq) * self.share, self.share
        if half is not None:
            count = self.share // 2
            start = start + half * count
        return self.view(pl.ds(pl.multiple_of(start, count), count))

    def send(self, ref, to, sem):
        pltpu.make_async_remote_copy(
            src_ref=ref, dst_ref=ref, send_sem=self.sems.at[16], recv_sem=self.sems.at[sem],
            device_id=(to, self.narrow), device_id_type=MESH,
        ).start()

    def got(self, ref, sem):
        pltpu.make_async_remote_copy(
            src_ref=ref, dst_ref=ref, send_sem=self.sems.at[16], recv_sem=self.sems.at[sem],
            device_id=(self.partner, self.narrow), device_id_type=MESH,
        ).wait_recv()

    def second(self, dp, k):
        ref = self.rows(dp, 0)
        self.send(ref, self.wide(0, 1), 3 + k)
        self.send(ref, self.wide(0, 3), 7 + k)
        self.send(ref, self.partner, 15)

    def own(self):
        ref = self.rows(0, 0)
        self.send(ref, self.wide(1, 0), 0)
        self.send(ref, self.wide(3, 0), 1)
        self.second(0, 0)

    def first_near(self):
        for side, (dp, to) in enumerate(((3, 1), (1, 3))):
            self.got(self.rows(dp, 0), side)
            self.send(self.rows(dp, 0, side), self.wide(to, 0), 2)
            self.second(dp, 1 + side)

    def first_far(self):
        self.got(self.rows(2, 0), 2)
        self.second(2, 3)

    def second_near(self, ks=(0, 1, 2, 3)):
        for k in ks:
            dp = (0, 3, 1, 2)[k]
            for side, (dq, to) in enumerate(((3, 1), (1, 3))):
                self.got(self.rows(dp, dq), 3 + 4 * side + k)
                self.send(self.rows(dp, dq, side), self.wide(0, to), 11 + k)
                self.send(self.rows(dp, dq), self.partner, 15)

    def second_far(self):
        for k, dp in enumerate((0, 3, 1, 2)):
            self.got(self.rows(dp, 2), 11 + k)
            self.send(self.rows(dp, 2), self.partner, 15)

    def last(self):
        self.got(self.view(pl.ds(0, 16 * self.share)), 15)

    def sent(self):
        ref = self.view(pl.ds(0, 31 * self.share))
        pltpu.make_async_remote_copy(
            src_ref=ref, dst_ref=ref, send_sem=self.sems.at[16], recv_sem=self.sems.at[15],
            device_id=(self.partner, self.narrow), device_id_type=MESH,
        ).wait_send()


def kernel(
    row_ref, col_ref, primal_ref, dual_ref, out_ref,
    rows_v, both_v, cols_v, prods_v, panel_v, aug, tile,
    first_hi, first_lo, slab_v, inv_hi, inv_lo, mid_hi, mid_lo, mix_hi, mix_lo,
    sems, z_sems, in_sems,
):
    wide, narrow = lax.axis_index("wide"), lax.axis_index("narrow")
    planes = lax.axis_size("narrow")
    order = rows_v.shape[1]
    panel = aug.shape[0]
    share = both_v.shape[0] // 2
    scale = 16.0 / (order * order)

    load_rows = pltpu.make_async_copy(row_ref, rows_v, in_sems.at[0])
    load_primal = pltpu.make_async_copy(primal_ref, both_v.at[pl.ds(0, share)], in_sems.at[1])
    load_dual = pltpu.make_async_copy(dual_ref, both_v.at[pl.ds(share, share)], in_sems.at[2])
    load_primal.start()
    load_dual.start()
    load_rows.start()

    mine = pl.ds(pl.multiple_of(wide * share, share), share)
    shard = col_ref[...]
    cols_v[1, mine, :] = shard

    @pl.when(narrow == 0)
    def _():
        cols_v[0, mine, :] = shard

    panel_cols = Gather(lambda r: cols_v.at[0, r], share, sems.at[0])
    block_cols = Gather(lambda r: cols_v.at[1, r], share, sems.at[1])
    panel_prods = Gather(lambda r: prods_v.at[0, :, r], share, sems.at[2])
    block_prods = Gather(lambda r: prods_v.at[1, :, r], share, sems.at[3])

    barrier = pltpu.get_barrier_semaphore()
    g = panel_cols
    for to in (g.wide(1, 0), g.wide(3, 0), g.wide(0, 1), g.wide(0, 3), g.partner):
        pl.semaphore_signal(barrier, inc=1, device_id=(to, narrow), device_id_type=MESH)

    @pl.when(narrow == 0)
    def _():
        for z in range(1, planes):
            pl.semaphore_signal(barrier, inc=1, device_id=(wide, z), device_id_type=MESH)
        pl.semaphore_wait(barrier, 5 + planes - 1)

    @pl.when(narrow != 0)
    def _():
        pl.semaphore_signal(barrier, inc=1, device_id=(wide, 0), device_id_type=MESH)
        pl.semaphore_wait(barrier, 6)

    def z_copy(z):
        ref = cols_v.at[0, mine]
        return pltpu.make_async_remote_copy(
            src_ref=ref, dst_ref=ref, send_sem=z_sems.at[0], recv_sem=z_sems.at[1],
            device_id=(wide, z), device_id_type=MESH,
        )

    @pl.when(narrow == 0)
    def _():
        for z in (4, 3, 5, 2, 6, 1, 7):
            z_copy(z).start()

    block_cols.own()
    block_cols.first_near()

    @pl.when(narrow != 0)
    def _():
        z_copy(0).wait_recv()

    panel_cols.own()
    block_cols.first_far()
    panel_cols.first_near()
    block_cols.second_near()
    panel_cols.first_far()
    block_cols.second_far()
    panel_cols.second_near()
    panel_cols.second_far()

    def products(which):
        done = dot(both_v[...], cols_v[which]).astype(BF16)
        prods_v[which, 0, mine, :] = done[:share]
        prods_v[which, 1, mine, :] = done[share:]

    load_primal.wait()
    load_dual.wait()
    panel_cols.last()
    products(0)
    panel_prods.own()
    block_cols.last()
    products(1)
    panel_prods.first_near()
    block_prods.own()

    def turn(t, _):
        at = pl.ds(pl.multiple_of(t * TILE, TILE), TILE)
        panel_v[:, at] = cols_v[0, at, :].T
        return 0

    lax.fori_loop(0, order // TILE, turn, 0)

    panel_prods.first_far()
    block_prods.first_near()
    panel_prods.second_near()
    block_prods.first_far()
    panel_prods.second_far()
    panel_prods.last()

    def hadamard(lhs, which):
        return dot(lhs, prods_v[which, 0]) * dot(lhs, prods_v[which, 1]) * scale

    step = 256

    def each(count, body):
        def one(t, _):
            body(pl.ds(pl.multiple_of(t * step, step), step))
            return 0

        lax.fori_loop(0, count // step, one, 0)

    @lambda body: each(panel, body)
    def _(at):
        aug[at, :] = hadamard(panel_v[at, :], 0)

    half = rows_v.shape[0] // 2
    blocks = panel // TILE

    def early(b, _):
        def beside():
            at = pl.ds(pl.multiple_of(b * half, half), half)
            first_hi[at, :], first_lo[at, :] = split(hadamard(rows_v[at, :], 0))

        factor_block(aug, tile, b, beside)

        @pl.when(b == 0)
        def _():
            block_prods.second_near()

        return 0

    def late(b, _):
        def beside():
            at = pl.ds(pl.multiple_of((b - blocks // 2) * half, half), half)
            slab_v[at, :] = hadamard(rows_v[at, :], 1)
            at = pl.ds(pl.multiple_of((b - blocks // 2) * (panel // 2), panel // 2), panel // 2)
            mix_hi[at, :], mix_lo[at, :] = split(hadamard(panel_v[at, :], 1))

        factor_block(aug, tile, b, beside)
        return 0

    load_rows.wait()
    lax.fori_loop(0, blocks // 2, early, 0)
    block_prods.second_far()
    block_prods.last()
    lax.fori_loop(blocks // 2, blocks, late, 0)

    for b in range(panel // TILE):
        at = pl.ds(b * TILE, TILE)
        lanes = lax.broadcasted_iota(jnp.int32, (TILE, panel), 1)
        kept = jnp.where(lanes < (b + 1) * TILE, aug[at, :], 0.0)
        inv_hi[at, :], inv_lo[at, :] = split(kept)

    @lambda body: each(panel, body)
    def _(at):
        solved = dot(inv_hi[at, :], mix_hi[...]) + (
            dot(inv_hi[at, :], mix_lo[...]) + dot(inv_lo[at, :], mix_hi[...])
        )
        rows = lax.broadcasted_iota(jnp.int32, (step, panel), 0) + at.start
        lanes = lax.broadcasted_iota(jnp.int32, (step, panel), 1)
        solved = jnp.where(narrow == 0, jnp.where(rows == lanes, -1.0, 0.0), solved)
        mid_hi[at, :], mid_lo[at, :] = split(solved)

    @lambda body: each(panel, body)
    def _(at):
        mixed = dot_first(inv_hi[:, at], mid_hi[...]) + (
            dot_first(inv_hi[:, at], mid_lo[...]) + dot_first(inv_lo[:, at], mid_hi[...])
        )
        mix_hi[at, :], mix_lo[at, :] = split(mixed)

    @lambda body: each(rows_v.shape[0], body)
    def _(at):
        taken = dot(first_hi[at, :], mix_hi[...]) + (
            dot(first_hi[at, :], mix_lo[...]) + dot(first_lo[at, :], mix_hi[...])
        )
        out_ref[at, :] = jnp.where(narrow == 0, 0.0, slab_v[at, :]) - taken


    for g in (block_cols, panel_cols, panel_prods, block_prods):
        g.sent()

    @pl.when(narrow == 0)
    def _():
        ref = cols_v.at[0, pl.ds(0, (planes - 1) * share)]
        pltpu.make_async_remote_copy(
            src_ref=ref, dst_ref=ref, send_sem=z_sems.at[0], recv_sem=z_sems.at[1],
            device_id=(wide, 1), device_id_type=MESH,
        ).wait_send()


def per_device(row_vectors, col_vectors, primal_matrix, dual_inverse):
    rows, order = row_vectors.shape
    panel = col_vectors.shape[0]
    share = primal_matrix.shape[0]
    whole = pl.BlockSpec(memory_space=pltpu.HBM)
    small, square = (panel, order), (panel, panel)
    return pl.pallas_call(
        kernel,
        out_shape=jax.ShapeDtypeStruct((rows, panel), F32),
        in_specs=[whole, pl.BlockSpec(memory_space=pltpu.VMEM), whole, whole],
        out_specs=pl.BlockSpec(memory_space=pltpu.VMEM),
        scratch_shapes=[
            pltpu.VMEM((rows, order), BF16),
            pltpu.VMEM((2 * share, order), BF16),
            pltpu.VMEM((2, order, panel), BF16),
            pltpu.VMEM((2, 2, order, panel), BF16),
            pltpu.VMEM(small, BF16),
            pltpu.VMEM(square, F32),
            pltpu.VMEM((TILE, TILE), F32),
            pltpu.VMEM((rows, panel), BF16),
            pltpu.VMEM((rows, panel), BF16),
            pltpu.VMEM((rows, panel), F32),
            *[pltpu.VMEM(square, BF16)] * 6,
            pltpu.SemaphoreType.DMA((4, 17)),
            pltpu.SemaphoreType.DMA((2,)),
            pltpu.SemaphoreType.DMA((3,)),
        ],
        compiler_params=pltpu.CompilerParams(
            collective_id=0, has_side_effects=True, vmem_limit_bytes=61 << 20
        ),
    )(row_vectors, col_vectors.T, primal_matrix, dual_inverse)


def solution(mesh):
    placed = (P("wide", None), P("narrow", "wide"), P("wide", None), P("wide", None))
    return jax.shard_map(
        per_device, mesh=mesh, in_specs=placed, out_specs=P("wide", "narrow"), check_vma=False
    )
```
